32 devices in a mesh: scan: 4 (over y, x), slab: 8 (over z, core).
Axes of the slice: x: 2, y: 2, z: 4, core: 2. Of those that a mesh axis runs over, the one named last changes fastest.
Arguments:
- solution: float32 [1536, 2048], P(('scan', 'slab')), parts along dimension 0, may hold values from -6 to 6
- direction: float32 [1536, 2048], P(('scan', 'slab')), parts along dimension 0, may hold values from -20 to 20
- gradient: float32 [1536, 2048], P(('scan', 'slab')), parts along dimension 0, may hold values from -40 to 40
- residual: float32 [512, 64, 896], P(('scan', 'slab')), parts along dimension 0, may hold values from -20 to 20
- tiles: bfloat16 [4, 2048, 896], replicated, may hold values from -0.125 to 0.125
- offsets: int32 [512], P(('scan', 'slab')), parts along dimension 0, may hold values from 1 to 320, as said below
Outputs:
- solution_next: float32 [1536, 2048], P(('scan', 'slab')), parts along dimension 0
- residual_next: float32 [512, 64, 896], P(('scan', 'slab')), parts along dimension 0
- gradient_next: float32 [1536, 2048], P(('scan', 'slab')), parts along dimension 0
- direction_next: float32 [1536, 2048], P(('scan', 'slab')), parts along dimension 0
The draws below stay inside these ranges and needn't reach their ends.
There are 4 independent parts, one for each index of `scan`. The reference program is written for one: setup_inputs(seed, part) draws one part's arguments, and reference() takes and returns one part's arrays. A program takes and returns all parts, laid end to end along the dimension named above; an argument that names none is the same for every part. Nothing has to cross between parts.
Inputs may be any that keep to these rules, and one draw needn't show every extreme that they name: View v belongs to slab v // 16, whose planes are s * 48 to s * 48 + 47 for slab s; its window offsets[v] to offsets[v] + 63 meets that slab and lies within the slab before it, the slab itself and the slab after it; offsets are 1 or more.
All inputs are finite; a program needn't handle non-finite values.
Results may differ from the reference program's by a relative error of at most 0.0029.
Values may be sent and summed in bfloat16 or wider, within the bound.
A program may use at most 192 MiB of HBM per device.

```python
import math
import jax
import jax.numpy as jnp
from jax import lax

ZD = 48
DR = 64
DC = 896
P_SIZE = 2048
VIEW_DEV = 16
ANGLES = 4
NZ = 384
VIEWS = 128


def rising_draw(key, length, inner_dims):
    positions = jnp.arange(length, dtype=jnp.float32) / max(length - 1, 1)
    rising_scale = jnp.exp(positions * math.log(3.0)).reshape((length,) + (1,) * len(inner_dims))
    values = jnp.clip(jax.random.normal(key, (length,) + inner_dims, jnp.float32), -4.0, 4.0)
    return values * rising_scale


def draw_direction(key, part):
    return rising_draw(jax.random.fold_in(key, 11), NZ, (P_SIZE,))


def draw_gradient(key, part):
    overall = jnp.exp(jax.random.uniform(jax.random.fold_in(key, 21), (), jnp.float32, math.log(0.5), math.log(2.0)))
    return rising_draw(jax.random.fold_in(key, 12), NZ, (P_SIZE,)) * overall


def draw_residual(key, part):
    return rising_draw(jax.random.fold_in(key, 13), VIEWS, (DR, DC))


def draw_offsets(key, part):
    owners = jnp.arange(VIEWS, dtype=jnp.int32) // VIEW_DEV
    lowest = jnp.maximum(jnp.maximum((owners - 1) * ZD, owners * ZD - DR + 1), 1)
    highest = jnp.minimum(jnp.minimum(owners * ZD + ZD - 1, (owners + 2) * ZD - DR), NZ - DR)
    return jax.random.randint(jax.random.fold_in(key, 14), (VIEWS,), lowest, highest + 1, jnp.int32)


def block_levels(rng, extent, cuts, smallest, high):
    gain, own = 1.0, jax.random.fold_in(rng, 6)
    for dim, shards_of in cuts:
        steps = jnp.exp(jax.random.uniform(jax.random.fold_in(own, dim), (shards_of,), jnp.float32, smallest / len(cuts), high / len(cuts)))
        gain = gain * jnp.repeat(steps, extent[dim] // shards_of).reshape([-1 if axis == dim else 1 for axis in range(len(extent))])
    return gain


def scatter_about(own_key, dims, width, most, shards=(), held_as=jnp.bfloat16):
    drawn = width * jax.random.normal(own_key, dims, jnp.float32)
    if shards:
        drawn = drawn * block_levels(own_key, dims, shards, -0.22, 0.18)
    return jnp.clip(drawn, -most, most).astype(held_as)


def setup_inputs(seed: int = 0, part: int = 0) -> dict:
    arg_keys = jax.random.split(jax.random.key(seed), 7)
    part_keys = jax.random.split(jax.random.fold_in(arg_keys[6], part), 7)
    solution = scatter_about(part_keys[0], (NZ, P_SIZE), 1.0, 6.0, ((0, 8),), jnp.float32)
    direction = draw_direction(jax.random.fold_in(jax.random.fold_in(arg_keys[6], part), 71), part)
    gradient = draw_gradient(jax.random.fold_in(jax.random.fold_in(arg_keys[6], part), 71), part)
    residual = draw_residual(jax.random.fold_in(jax.random.fold_in(arg_keys[6], part), 71), part)
    tiles = scatter_about(arg_keys[4], (ANGLES, P_SIZE, DC), P_SIZE ** -0.5, 0.125)
    offsets = draw_offsets(jax.random.fold_in(jax.random.fold_in(arg_keys[6], part), 71), part)
    return dict(solution=solution, direction=direction, gradient=gradient, residual=residual, tiles=tiles, offsets=offsets)


def reference(solution, direction, gradient, residual, tiles, offsets):
    direction_half = direction.astype(jnp.bfloat16)
    view_total = offsets.shape[0]
    angle_ids = (jnp.arange(view_total, dtype=jnp.int32) % ANGLES).astype(jnp.int32)

    def forward_view(carried, view_item):
        first_row, angle_index = view_item
        window_rows = lax.dynamic_slice_in_dim(direction_half, first_row.astype(jnp.int32), DR, 0)
        angle_tile = lax.dynamic_index_in_dim(tiles, angle_index, 0, keepdims=False)
        return carried, jnp.dot(window_rows, angle_tile, preferred_element_type=jnp.float32)

    _, projected = lax.scan(forward_view, jnp.float32(0.0), (offsets, angle_ids))
    grad_norm = jnp.sum(gradient * gradient)
    image_norm = jnp.sum(projected * projected)
    step_size = grad_norm / image_norm
    solution_next = solution + step_size * direction
    residual_next = residual - step_size * projected
    residual_half = residual_next.astype(jnp.bfloat16)

    def backward_view(accumulated, view_item):
        first_row, angle_index, residual_rows = view_item
        angle_tile = lax.dynamic_index_in_dim(tiles, angle_index, 0, keepdims=False)
        contribution = lax.dot_general(residual_rows, angle_tile, (((1,), (1,)), ((), ())), preferred_element_type=jnp.float32)
        first_row = first_row.astype(jnp.int32)
        current = lax.dynamic_slice_in_dim(accumulated, first_row, DR, 0)
        return lax.dynamic_update_slice_in_dim(accumulated, current + contribution, first_row, 0), None

    empty = jnp.zeros((NZ, P_SIZE), jnp.float32)
    gradient_next, _ = lax.scan(backward_view, empty, (offsets, angle_ids, residual_half))
    new_norm = jnp.sum(gradient_next * gradient_next)
    direction_next = gradient_next + (new_norm / grad_norm) * direction
    return solution_next, residual_next, gradient_next, direction_next
```

```python
import functools

import jax
import jax.numpy as jnp
from jax import lax
from jax.experimental import pallas as pl
from jax.experimental.pallas import tpu as pltpu
from jax.sharding import PartitionSpec as P

LANES = 128
STATS = 5
PROJECT_MIB = 30
FINISH_MIB = 8


def fold(value):
    total = value[:, :LANES]
    for start in range(LANES, value.shape[1], LANES):
        total = total + value[:, start : start + LANES]
    return jnp.sum(total, axis=0, keepdims=True)


def split(value):
    upper = value.astype(jnp.bfloat16)
    return upper, (value - upper.astype(jnp.float32)).astype(jnp.bfloat16)


def project(
    count,
    offsets_hbm,
    direction_hbm,
    gradient_hbm,
    residual_hbm,
    tiles_hbm,
    residual_vm,
    direction_vm,
    images,
    back_image,
    back_residual,
    stats_out,
    offsets_sm,
    gradient_vm,
    tiles_vm,
    own,
    halo,
    hits,
    covers,
    covers_in,
    sums_own,
    sums_out,
    sums_in,
    stacked,
    total,
    stat_send,
    stat_recv,
    load_sems,
    residual_sems,
    tile_sems,
    cover_send,
    cover_recv,
    sums_send,
    sums_recv,
    halo_send,
    halo_recv,
    stat_send_sems,
    stat_recv_sems,
):
    me = lax.axis_index("slab")
    planes, cells = direction_vm.shape
    angles, per_angle, rows, columns = residual_vm.shape
    near = 3 * planes
    f32, bf16 = jnp.float32, jnp.bfloat16
    has_low = me > 0
    has_high = me < count - 1
    low = {"slab": lax.rem(me + count - 1, count)}
    high = {"slab": lax.rem(me + 1, count)}

    load_offsets = pltpu.make_async_copy(offsets_hbm, offsets_sm, load_sems.at[0])
    load_direction = pltpu.make_async_copy(direction_hbm, direction_vm, load_sems.at[1])
    load_gradient = pltpu.make_async_copy(gradient_hbm, gradient_vm, load_sems.at[2])

    def load_residual(a):
        return pltpu.make_async_copy(residual_hbm.at[:, a], residual_vm.at[a], residual_sems.at[a])

    def load_tile(a):
        return pltpu.make_async_copy(tiles_hbm.at[a], tiles_vm.at[a], tile_sems.at[a])

    load_offsets.start()
    load_direction.start()
    for a in range(angles):
        load_residual(a).start()
    for a in range(angles):
        load_tile(a).start()
    load_gradient.start()

    barrier = pltpu.get_barrier_semaphore()
    for d in range(1, count):
        pl.semaphore_signal(barrier, inc=1, device_id={"slab": lax.rem(me + d, count)})

    @pl.when(jnp.logical_not(has_low))
    def _():
        halo[:planes, :] = jnp.zeros((planes, cells), bf16)
        covers_in[0] = jnp.zeros((planes, LANES), bf16)
        sums_in[:, 0] = jnp.zeros((angles, planes, columns), bf16)

    @pl.when(jnp.logical_not(has_high))
    def _():
        halo[planes:, :] = jnp.zeros((planes, cells), bf16)
        covers_in[1] = jnp.zeros((planes, LANES), bf16)
        sums_in[:, 1] = jnp.zeros((angles, planes, columns), bf16)

    load_offsets.wait()
    shift = planes - me * planes

    lane = lax.broadcasted_iota(jnp.int32, (near, LANES), 1)
    plane = lax.broadcasted_iota(jnp.int32, (near, LANES), 0)
    first = jnp.full((near, LANES), near, jnp.int32)
    for v in range(angles * per_angle):
        first = jnp.where(lane == v, offsets_sm[v] + shift, first)
    inside = jnp.logical_and(plane >= first, plane < first + rows)
    covers[...] = jnp.where(inside, 1.0, 0.0).astype(bf16)

    plane_id = lax.broadcasted_iota(jnp.int32, (near, per_angle * rows), 0)
    row_id = lax.broadcasted_iota(jnp.int32, (near, per_angle * rows), 1)
    for a in range(angles):
        base = jnp.zeros_like(row_id)
        for j in range(per_angle):
            base = jnp.where(row_id >= j * rows, offsets_sm[j * angles + a] + shift - j * rows, base)
        hits[a] = jnp.where(plane_id == row_id + base, 1.0, 0.0).astype(bf16)

    load_direction.wait()
    own[...] = direction_vm[...].astype(bf16)

    def cover_copy(side):
        source = covers.at[pl.ds(0 if side == 0 else 2 * planes, planes)]
        return pltpu.make_async_remote_copy(
            source, covers_in.at[1 - side], cover_send.at[side], cover_recv.at[1 - side],
            device_id=low if side == 0 else high,
        )

    def sums_copy(side, a):
        return pltpu.make_async_remote_copy(
            sums_out.at[a, side], sums_in.at[a, 1 - side], sums_send.at[side, a], sums_recv.at[1 - side, a],
            device_id=low if side == 0 else high,
        )

    def halo_copy(side):
        return pltpu.make_async_remote_copy(
            own, halo.at[pl.ds((1 - side) * planes, planes)], halo_send.at[side], halo_recv.at[1 - side],
            device_id=low if side == 0 else high,
        )

    pl.semaphore_wait(barrier, count - 1)

    @pl.when(has_low)
    def _():
        cover_copy(0).start()

    @pl.when(has_high)
    def _():
        cover_copy(1).start()

    def gather_rows(a, carry):
        load_residual(a).wait()
        upper, lower = split(residual_vm[a].reshape(per_angle * rows, columns))
        sums = jnp.dot(hits[a], upper, preferred_element_type=f32) + jnp.dot(
            hits[a], lower, preferred_element_type=f32
        )
        sums_own[a] = sums[planes : 2 * planes]
        sums_out[a, 0] = sums[:planes].astype(bf16)
        sums_out[a, 1] = sums[2 * planes :].astype(bf16)

        @pl.when(has_low)
        def _():
            sums_copy(0, a).start()

        @pl.when(has_high)
        def _():
            sums_copy(1, a).start()

        return carry

    lax.fori_loop(0, angles, gather_rows, 0)

    @pl.when(has_low)
    def _():
        halo_copy(0).start()
        cover_copy(0).wait_send()
        cover_copy(1).wait_recv()

    @pl.when(has_high)
    def _():
        halo_copy(1).start()
        cover_copy(1).wait_send()
        cover_copy(0).wait_recv()

    covered = covers[planes : 2 * planes].astype(f32) + covers_in[0].astype(f32) + covers_in[1].astype(f32)
    covered = covered.astype(bf16)
    view_of = lax.broadcasted_iota(jnp.int32, (LANES, LANES), 0)

    def forward(a, image_part):
        chosen = jnp.where(lax.rem(view_of, angles) == a, 1.0, 0.0).astype(bf16)
        times = jnp.dot(covered, chosen, preferred_element_type=f32)
        load_tile(a).wait()
        image = jnp.dot(own[...], tiles_vm[a], preferred_element_type=f32)
        for l in range(columns // LANES):
            cut = slice(l * LANES, (l + 1) * LANES)
            piece = image[:, cut]
            weighted = times * piece
            images[a, l, planes : 2 * planes] = piece
            stacked[a, :planes, cut] = weighted.astype(bf16)
            image_part = image_part + jnp.sum(weighted * piece, axis=0, keepdims=True)
        return image_part

    image_part = lax.fori_loop(0, angles, forward, jnp.zeros((1, LANES), f32))

    def backward(a, carry):
        @pl.when(has_low)
        def _():
            sums_copy(1, a).wait_recv()

        @pl.when(has_high)
        def _():
            sums_copy(0, a).wait_recv()

        sums = sums_own[a] + sums_in[a, 0].astype(f32) + sums_in[a, 1].astype(f32)
        upper, lower = split(sums)
        stacked[a, planes : 2 * planes] = upper
        stacked[a, 2 * planes :] = lower
        part = lax.dot_general(
            stacked[a], tiles_vm[a], (((1,), (1,)), ((), ())), preferred_element_type=f32
        )

        @pl.when(a == 0)
        def _():
            total[...] = part

        @pl.when(a > 0)
        def _():
            total[...] = total[...] + part

        return carry

    lax.fori_loop(0, angles, backward, 0)

    from_image = total[:planes]
    from_residual = total[planes : 2 * planes] + total[2 * planes :]
    back_image[...] = from_image
    back_residual[...] = from_residual
    load_gradient.wait()
    gradient = gradient_vm[...]
    stat_send[...] = jnp.concatenate(
        [
            fold(gradient * gradient),
            image_part,
            fold(from_residual * from_residual),
            fold(from_residual * from_image),
            fold(from_image * from_image),
            jnp.zeros((8 - STATS, LANES), f32),
        ],
        axis=0,
    )
    copies = []
    for d in range(1, count):
        copies.append(
            pltpu.make_async_remote_copy(
                stat_send, stat_recv.at[d], stat_send_sems.at[d], stat_recv_sems.at[d],
                device_id={"slab": lax.rem(me + d, count)},
            )
        )
    for copy in copies:
        copy.start()

    @pl.when(has_low)
    def _():
        halo_copy(0).wait_send()
        halo_copy(1).wait_recv()

    @pl.when(has_high)
    def _():
        halo_copy(1).wait_send()
        halo_copy(0).wait_recv()

    def forward_halo(a, carry):
        image = jnp.dot(halo[...], tiles_vm[a], preferred_element_type=f32)
        for l in range(columns // LANES):
            cut = slice(l * LANES, (l + 1) * LANES)
            images[a, l, :planes] = image[:planes, cut]
            images[a, l, 2 * planes :] = image[planes:, cut]
        return carry

    lax.fori_loop(0, angles, forward_halo, 0)

    @pl.when(has_low)
    def _():
        for a in range(angles):
            sums_copy(0, a).wait_send()

    @pl.when(has_high)
    def _():
        for a in range(angles):
            sums_copy(1, a).wait_send()

    sums = stat_send[...]
    for d, copy in enumerate(copies):
        copy.wait()
        sums = sums + stat_recv[d + 1]
    norms = jnp.sum(sums, axis=1, keepdims=True)
    grad_norm, image_norm = norms[0:1], norms[1:2]
    step_size = grad_norm / image_norm
    new_norm = norms[2:3] - 2.0 * step_size * norms[3:4] + step_size * step_size * norms[4:5]
    stats_out[...] = jnp.concatenate(
        [
            jnp.broadcast_to(step_size, (1, LANES)),
            jnp.broadcast_to(new_norm / grad_norm, (1, LANES)),
            jnp.zeros((6, LANES), f32),
        ],
        axis=0,
    )


def finish(
    offsets_ref, stats, solution_ref, direction_ref, back_image, back_residual, images, residual_ref,
    solution_out, residual_out, gradient_out, direction_out,
    solution_vm, gradient_vm, direction_vm, residual_vm, sems, residual_sems,
):
    me = lax.axis_index("slab")
    planes = direction_ref.shape[0]
    angles, per_angle, rows, columns = residual_ref.shape
    step_size = stats[0:1, 0:1]
    scale = stats[1:2, 0:1]
    stores = [
        pltpu.make_async_copy(gradient_vm, gradient_out, sems.at[0]),
        pltpu.make_async_copy(direction_vm, direction_out, sems.at[1]),
        pltpu.make_async_copy(solution_vm, solution_out, sems.at[2]),
    ]
    gradient = back_residual[...] - step_size * back_image[...]
    gradient_vm[...] = gradient
    stores[0].start()
    direction_vm[...] = gradient + scale * direction_ref[...]
    stores[1].start()
    solution_vm[...] = solution_ref[...] + step_size * direction_ref[...]
    stores[2].start()

    def store_view(j, a):
        return pltpu.make_async_copy(residual_vm.at[j, a], residual_out.at[j, a], residual_sems.at[j, a])

    shift = planes - me * planes
    for j in range(per_angle):
        for a in range(angles):
            first = offsets_ref[j * angles + a] + shift
            for l in range(columns // LANES):
                cut = slice(l * LANES, (l + 1) * LANES)
                window = images[a, l, pl.ds(first, rows), :]
                residual_vm[j, a, :, cut] = residual_ref[a, j, :, cut] - step_size * window
            store_view(j, a).start()
    for store in stores:
        store.wait()
    for j in range(per_angle):
        for a in range(angles):
            store_view(j, a).wait()


def local(count, solution, direction, gradient, residual, tiles, offsets):
    planes, cells = solution.shape
    views, rows, columns = residual.shape
    angles = tiles.shape[0]
    per_angle = views // angles
    near = 3 * planes
    f32, bf16 = jnp.float32, jnp.bfloat16
    hbm = pl.BlockSpec(memory_space=pltpu.HBM)
    vmem = pl.BlockSpec(memory_space=pltpu.VMEM)
    smem = pl.BlockSpec(memory_space=pltpu.SMEM)
    dma = pltpu.SemaphoreType.DMA
    by_angle = residual.reshape(per_angle, angles, rows, columns)
    volume = jax.ShapeDtypeStruct((planes, cells), f32)
    remote = [pltpu.with_memory_space_constraint(x, pltpu.HBM) for x in (offsets, direction, gradient, by_angle, tiles)]
    residual_in, direction_in, images, back_image, back_residual, stats = pl.pallas_call(
        functools.partial(project, count),
        name="project",
        out_shape=(
            jax.ShapeDtypeStruct((angles, per_angle, rows, columns), f32),
            volume,
            jax.ShapeDtypeStruct((angles, columns // LANES, near, LANES), f32),
            volume,
            volume,
            jax.ShapeDtypeStruct((8, LANES), f32),
        ),
        in_specs=[hbm] * 5,
        out_specs=(vmem,) * 6,
        scratch_shapes=[
            pltpu.SMEM((views,), jnp.int32),
            pltpu.VMEM((planes, cells), f32),
            pltpu.VMEM((angles, cells, columns), bf16),
            pltpu.VMEM((planes, cells), bf16),
            pltpu.VMEM((2 * planes, cells), bf16),
            pltpu.VMEM((angles, near, per_angle * rows), bf16),
            pltpu.VMEM((near, LANES), bf16),
            pltpu.VMEM((2, planes, LANES), bf16),
            pltpu.VMEM((angles, planes, columns), f32),
            pltpu.VMEM((angles, 2, planes, columns), bf16),
            pltpu.VMEM((angles, 2, planes, columns), bf16),
            pltpu.VMEM((angles, near, columns), bf16),
            pltpu.VMEM((near, cells), f32),
            pltpu.VMEM((8, LANES), f32),
            pltpu.VMEM((count, 8, LANES), f32),
            dma((3,)),
            dma((angles,)),
            dma((angles,)),
            dma((2,)),
            dma((2,)),
            dma((2, angles)),
            dma((2, angles)),
            dma((2,)),
            dma((2,)),
            dma((count,)),
            dma((count,)),
        ],
        compiler_params=pltpu.CompilerParams(
            collective_id=0, has_side_effects=True, vmem_limit_bytes=PROJECT_MIB * 1024 * 1024
        ),
    )(*remote)
    results = pl.pallas_call(
        finish,
        name="finish",
        out_shape=(volume, jax.ShapeDtypeStruct((per_angle, angles, rows, columns), f32), volume, volume),
        in_specs=[smem] + [vmem] * 7,
        out_specs=(hbm,) * 4,
        scratch_shapes=[
            pltpu.VMEM((planes, cells), f32),
            pltpu.VMEM((planes, cells), f32),
            pltpu.VMEM((planes, cells), f32),
            pltpu.VMEM((per_angle, angles, rows, columns), f32),
            dma((3,)),
            dma((per_angle, angles)),
        ],
        compiler_params=pltpu.CompilerParams(vmem_limit_bytes=FINISH_MIB * 1024 * 1024),
    )(offsets, stats, solution, direction_in, back_image, back_residual, images, residual_in)
    return results[0], results[1].reshape(residual.shape), results[2], results[3]


def solution(mesh):
    placed = (
        P(("scan", "slab"), None),
        P(("scan", "slab"), None),
        P(("scan", "slab"), None),
        P(("scan", "slab"), None, None),
        P(),
        P(("scan", "slab")),
    )
    return jax.shard_map(
        functools.partial(local, mesh.shape["slab"]),
        mesh=mesh,
        in_specs=placed,
        out_specs=(
            P(("scan", "slab"), None),
            P(("scan", "slab"), None, None),
            P(("scan", "slab"), None),
            P(("scan", "slab"), None),
        ),
        check_vma=False,
    )
```

```python
import functools

import jax
import jax.numpy as jnp
from jax import lax
from jax.experimental import pallas as pl
from jax.experimental.pallas import tpu as pltpu
from jax.sharding import PartitionSpec as P

LANES = 128
STATS = 5
PROJECT_MIB = 30
FINISH_MIB = 8


def split(value):
    upper = value.astype(jnp.bfloat16)
    return upper, (value - upper.astype(jnp.float32)).astype(jnp.bfloat16)


def fold_tile(value):
    total = None
    for r in range(0, value.shape[0], 8):
        for c in range(0, value.shape[1], LANES):
            tile = value[r : r + 8, c : c + LANES]
            total = tile if total is None else total + tile
    return total


def project(
    count,
    offsets_hbm,
    direction_hbm,
    gradient_hbm,
    residual_hbm,
    tiles_hbm,
    residual_vm,
    direction_vm,
    images,
    back_image,
    back_residual,
    stats_out,
    offsets_sm,
    gradient_vm,
    tiles_vm,
    own,
    halo,
    hits,
    covers,
    covers_in,
    sums_own,
    sums_out,
    sums_in,
    stacked,
    partial,
    stat_send,
    stat_recv,
    load_sems,
    residual_sems,
    tile_sems,
    cover_send,
    cover_recv,
    sums_send,
    sums_recv,
    halo_send,
    halo_recv,
    stat_send_sems,
    stat_recv_sems,
):
    scope = jax.named_scope
    me = lax.axis_index("slab")
    planes, cells = direction_vm.shape
    angles, per_angle, rows, columns = residual_vm.shape
    near = 3 * planes
    f32, bf16 = jnp.float32, jnp.bfloat16
    has_low = me > 0
    has_high = me < count - 1
    low = {"slab": lax.rem(me + count - 1, count)}
    high = {"slab": lax.rem(me + 1, count)}

    load_offsets = pltpu.make_async_copy(offsets_hbm, offsets_sm, load_sems.at[0])
    load_direction = pltpu.make_async_copy(direction_hbm, direction_vm, load_sems.at[1])
    load_gradient = pltpu.make_async_copy(gradient_hbm, gradient_vm, load_sems.at[2])

    def load_residual(a):
        return pltpu.make_async_copy(residual_hbm.at[:, a], residual_vm.at[a], residual_sems.at[a])

    def load_tile(a):
        return pltpu.make_async_copy(tiles_hbm.at[a], tiles_vm.at[a], tile_sems.at[a])

    load_offsets.start()
    for a in range(angles):
        load_residual(a).start()
    load_direction.start()
    for a in range(angles):
        load_tile(a).start(priority=1)
    load_gradient.start(priority=1)

    barrier = pltpu.get_barrier_semaphore()
    for d in range(1, count):
        pl.semaphore_signal(barrier, inc=1, device_id={"slab": lax.rem(me + d, count)})

    @pl.when(jnp.logical_not(has_low))
    def _():
        halo[:planes, :] = jnp.zeros((planes, cells), bf16)
        covers_in[0] = jnp.zeros((planes, LANES), bf16)
        sums_in[:, 0] = jnp.zeros((angles, planes, columns), bf16)

    @pl.when(jnp.logical_not(has_high))
    def _():
        halo[planes:, :] = jnp.zeros((planes, cells), bf16)
        covers_in[1] = jnp.zeros((planes, LANES), bf16)
        sums_in[:, 1] = jnp.zeros((angles, planes, columns), bf16)

    with scope("w_off"):
        load_offsets.wait()
    shift = planes - me * planes

    lane = lax.broadcasted_iota(jnp.int32, (near, LANES), 1)
    plane = lax.broadcasted_iota(jnp.int32, (near, LANES), 0)
    first = jnp.full((near, LANES), near, jnp.int32)
    for v in range(angles * per_angle):
        first = jnp.where(lane == v, offsets_sm[v] + shift, first)
    inside = jnp.logical_and(plane >= first, plane < first + rows)
    covers[...] = jnp.where(inside, 1.0, 0.0).astype(bf16)

    plane_id = lax.broadcasted_iota(jnp.int32, (near, per_angle * rows), 0)
    row_id = lax.broadcasted_iota(jnp.int32, (near, per_angle * rows), 1)
    for a in range(angles):
        base = jnp.zeros_like(row_id)
        for j in range(per_angle):
            base = jnp.where(row_id >= j * rows, offsets_sm[j * angles + a] + shift - j * rows, base)
        hits[a] = jnp.where(plane_id == row_id + base, 1.0, 0.0).astype(bf16)

    def cover_copy(side):
        source = covers.at[pl.ds(0 if side == 0 else 2 * planes, planes)]
        return pltpu.make_async_remote_copy(
            source, covers_in.at[1 - side], cover_send.at[side], cover_recv.at[1 - side],
            device_id=low if side == 0 else high,
        )

    def sums_copy(side, a):
        return pltpu.make_async_remote_copy(
            sums_out.at[a, side], sums_in.at[a, 1 - side], sums_send.at[side, a], sums_recv.at[1 - side, a],
            device_id=low if side == 0 else high,
        )

    def halo_copy(side):
        return pltpu.make_async_remote_copy(
            own, halo.at[pl.ds((1 - side) * planes, planes)], halo_send.at[side], halo_recv.at[1 - side],
            device_id=low if side == 0 else high,
        )

    for a in range(angles):
        with scope("w_res"):
            load_residual(a).wait()
        upper, lower = split(residual_vm[a].reshape(per_angle * rows, columns))
        sums = jnp.dot(hits[a], upper, preferred_element_type=f32) + jnp.dot(
            hits[a], lower, preferred_element_type=f32
        )
        sums_own[a] = sums[planes : 2 * planes]
        sums_out[a, 0] = sums[:planes].astype(bf16)
        sums_out[a, 1] = sums[2 * planes :].astype(bf16)
        if a == 0:
            with scope("w_bar"):
                pl.semaphore_wait(barrier, count - 1)

        @pl.when(has_low)
        def _():
            if a == 0:
                cover_copy(0).start()
            sums_copy(0, a).start()

        @pl.when(has_high)
        def _():
            if a == 0:
                cover_copy(1).start()
            sums_copy(1, a).start()

    with scope("w_dir"):
        load_direction.wait()
    own[...] = direction_vm[...].astype(bf16)

    @pl.when(has_low)
    def _():
        halo_copy(0).start()

    @pl.when(has_high)
    def _():
        halo_copy(1).start()

    view_of = lax.broadcasted_iota(jnp.int32, (LANES, angles * LANES), 0)
    lane_of = lax.broadcasted_iota(jnp.int32, (LANES, angles * LANES), 1)
    chosen = jnp.where(lax.rem(view_of, angles) == lane_of // LANES, 1.0, 0.0).astype(bf16)
    image_sums = jnp.zeros((8, LANES), f32)
    product_sums = [jnp.zeros((8, LANES), f32)] * 3
    times = None

    def backward(first_angle, last_angle):
        chunk = 2 * LANES
        for p in range(0, cells, chunk):
            part = None
            for a in range(first_angle, last_angle):
                product = lax.dot_general(
                    tiles_vm[a, p : p + chunk], stacked[a], (((1,), (1,)), ((), ())), preferred_element_type=f32
                )
                part = product if part is None else part + product
            if first_angle > 0:
                part = part + partial[p : p + chunk]
            if last_angle < angles:
                partial[p : p + chunk] = part
                continue
            turned = part.T
            from_image, from_residual = turned[:planes], turned[planes:]
            back_image[:, p : p + chunk] = from_image
            back_residual[:, p : p + chunk] = from_residual
            product_sums[0] = product_sums[0] + fold_tile(from_residual * from_residual)
            product_sums[1] = product_sums[1] + fold_tile(from_residual * from_image)
            product_sums[2] = product_sums[2] + fold_tile(from_image * from_image)

    half = angles // 2
    for a in range(angles):
        with scope("w_tile"):
            load_tile(a).wait()
        if a == 0:
            with scope("w_cov"):
                @pl.when(has_low)
                def _():
                    cover_copy(0).wait_send()
                    cover_copy(1).wait_recv()

                @pl.when(has_high)
                def _():
                    cover_copy(1).wait_send()
                    cover_copy(0).wait_recv()

            covered = covers[planes : 2 * planes].astype(f32) + covers_in[0].astype(f32) + covers_in[1].astype(f32)
            times = jnp.dot(covered.astype(bf16), chosen, preferred_element_type=f32)
        image = jnp.dot(own[...], tiles_vm[a], preferred_element_type=f32)
        for l in range(columns // LANES):
            cut = slice(l * LANES, (l + 1) * LANES)
            piece = image[:, cut]
            weighted = times[:, a * LANES : (a + 1) * LANES] * piece
            images[a, l, planes : 2 * planes] = piece
            stacked[a, :planes, cut] = weighted.astype(bf16)
            image_sums = image_sums + fold_tile(weighted * piece)
        ready = range(0, half) if a == half else range(half, angles) if a == angles - 1 else ()
        if not ready:
            continue
        if a == angles - 1:
            with scope("w_grad"):
                load_gradient.wait()
            gradient_sums = fold_tile(gradient_vm[...] * gradient_vm[...])
        for b in ready:
            with scope("w_sums"):
                @pl.when(has_low)
                def _():
                    sums_copy(1, b).wait_recv()

                @pl.when(has_high)
                def _():
                    sums_copy(0, b).wait_recv()

            sums = sums_own[b] + sums_in[b, 0].astype(f32) + sums_in[b, 1].astype(f32)
            stacked[b, planes:] = sums.astype(bf16)
        with scope("bwd"):
            backward(ready[0], ready[-1] + 1)

    stat_send[...] = jnp.concatenate(
        [jnp.sum(x, axis=0, keepdims=True) for x in [gradient_sums, image_sums] + product_sums]
        + [jnp.zeros((8 - STATS, LANES), f32)],
        axis=0,
    )
    copies = []
    for d in range(1, count):
        copies.append(
            pltpu.make_async_remote_copy(
                stat_send, stat_recv.at[d], stat_send_sems.at[d], stat_recv_sems.at[d],
                device_id={"slab": lax.rem(me + d, count)},
            )
        )
    for copy in copies:
        copy.start()

    with scope("w_halo"):
        @pl.when(has_low)
        def _():
            halo_copy(0).wait_send()
            halo_copy(1).wait_recv()

        @pl.when(has_high)
        def _():
            halo_copy(1).wait_send()
            halo_copy(0).wait_recv()

    with scope("fwdhalo"):
        for a in range(angles):
            image = jnp.dot(halo[...], tiles_vm[a], preferred_element_type=f32)
            for l in range(columns // LANES):
                cut = slice(l * LANES, (l + 1) * LANES)
                images[a, l, :planes] = image[:planes, cut]
                images[a, l, 2 * planes :] = image[planes:, cut]

    @pl.when(has_low)
    def _():
        for a in range(angles):
            sums_copy(0, a).wait_send()

    @pl.when(has_high)
    def _():
        for a in range(angles):
            sums_copy(1, a).wait_send()

    with scope("w_stat"):
        for copy in copies:
            copy.wait()
    with scope("stat"):
        sums = stat_send[...]
        for d in range(1, count):
            sums = sums + stat_recv[d]
        norms = jnp.sum(sums, axis=1, keepdims=True)
        grad_norm, image_norm = norms[0:1], norms[1:2]
        step_size = grad_norm / image_norm
        new_norm = norms[2:3] - 2.0 * step_size * norms[3:4] + step_size * step_size * norms[4:5]
        stats_out[...] = jnp.concatenate(
            [
                jnp.broadcast_to(step_size, (1, LANES)),
                jnp.broadcast_to(new_norm / grad_norm, (1, LANES)),
                jnp.zeros((6, LANES), f32),
            ],
            axis=0,
        )


def finish(
    offsets_ref, stats, solution_ref, direction_ref, back_image, back_residual, images, residual_ref,
    solution_out, residual_out, gradient_out, direction_out,
    solution_vm, gradient_vm, direction_vm, residual_vm, sems, residual_sems,
):
    me = lax.axis_index("slab")
    planes = direction_ref.shape[0]
    angles, per_angle, rows, columns = residual_ref.shape
    step_size = stats[0:1, 0:1]
    scale = stats[1:2, 0:1]
    stores = [
        pltpu.make_async_copy(gradient_vm, gradient_out, sems.at[0]),
        pltpu.make_async_copy(direction_vm, direction_out, sems.at[1]),
        pltpu.make_async_copy(solution_vm, solution_out, sems.at[2]),
    ]
    gradient = back_residual[...] - step_size * back_image[...]
    gradient_vm[...] = gradient
    stores[0].start()
    direction_vm[...] = gradient + scale * direction_ref[...]
    stores[1].start()
    solution_vm[...] = solution_ref[...] + step_size * direction_ref[...]
    stores[2].start()

    def store_view(j, a):
        return pltpu.make_async_copy(residual_vm.at[j, a], residual_out.at[j, a], residual_sems.at[j, a])

    shift = planes - me * planes
    for j in range(per_angle):
        for a in range(angles):
            first = offsets_ref[j * angles + a] + shift
            for l in range(columns // LANES):
                cut = slice(l * LANES, (l + 1) * LANES)
                window = images[a, l, pl.ds(first, rows), :]
                residual_vm[j, a, :, cut] = residual_ref[a, j, :, cut] - step_size * window
            store_view(j, a).start()
    for store in stores:
        store.wait()
    for j in range(per_angle):
        for a in range(angles):
            store_view(j, a).wait()


def local(count, solution, direction, gradient, residual, tiles, offsets):
    planes, cells = solution.shape
    views, rows, columns = residual.shape
    angles = tiles.shape[0]
    per_angle = views // angles
    near = 3 * planes
    f32, bf16 = jnp.float32, jnp.bfloat16
    hbm = pl.BlockSpec(memory_space=pltpu.HBM)
    vmem = pl.BlockSpec(memory_space=pltpu.VMEM)
    smem = pl.BlockSpec(memory_space=pltpu.SMEM)
    dma = pltpu.SemaphoreType.DMA
    by_angle = residual.reshape(per_angle, angles, rows, columns)
    volume = jax.ShapeDtypeStruct((planes, cells), f32)
    remote = [pltpu.with_memory_space_constraint(x, pltpu.HBM) for x in (offsets, direction, gradient, by_angle, tiles)]
    residual_in, direction_in, images, back_image, back_residual, stats = pl.pallas_call(
        functools.partial(project, count),
        name="project",
        out_shape=(
            jax.ShapeDtypeStruct((angles, per_angle, rows, columns), f32),
            volume,
            jax.ShapeDtypeStruct((angles, columns // LANES, near, LANES), f32),
            volume,
            volume,
            jax.ShapeDtypeStruct((8, LANES), f32),
        ),
        in_specs=[hbm] * 5,
        out_specs=(vmem,) * 6,
        scratch_shapes=[
            pltpu.SMEM((views,), jnp.int32),
            pltpu.VMEM((planes, cells), f32),
            pltpu.VMEM((angles, cells, columns), bf16),
            pltpu.VMEM((planes, cells), bf16),
            pltpu.VMEM((2 * planes, cells), bf16),
            pltpu.VMEM((angles, near, per_angle * rows), bf16),
            pltpu.VMEM((near, LANES), bf16),
            pltpu.VMEM((2, planes, LANES), bf16),
            pltpu.VMEM((angles, planes, columns), f32),
            pltpu.VMEM((angles, 2, planes, columns), bf16),
            pltpu.VMEM((angles, 2, planes, columns), bf16),
            pltpu.VMEM((angles, 2 * planes, columns), bf16),
            pltpu.VMEM((cells, 2 * planes), f32),
            pltpu.VMEM((8, LANES), f32),
            pltpu.VMEM((count, 8, LANES), f32),
            dma((3,)),
            dma((angles,)),
            dma((angles,)),
            dma((2,)),
            dma((2,)),
            dma((2, angles)),
            dma((2, angles)),
            dma((2,)),
            dma((2,)),
            dma((count,)),
            dma((count,)),
        ],
        compiler_params=pltpu.CompilerParams(
            collective_id=0, has_side_effects=True, vmem_limit_bytes=PROJECT_MIB * 1024 * 1024
        ),
    )(*remote)
    results = pl.pallas_call(
        finish,
        name="finish",
        out_shape=(volume, jax.ShapeDtypeStruct((per_angle, angles, rows, columns), f32), volume, volume),
        in_specs=[smem] + [vmem] * 7,
        out_specs=(hbm,) * 4,
        scratch_shapes=[
            pltpu.VMEM((planes, cells), f32),
            pltpu.VMEM((planes, cells), f32),
            pltpu.VMEM((planes, cells), f32),
            pltpu.VMEM((per_angle, angles, rows, columns), f32),
            dma((3,)),
            dma((per_angle, angles)),
        ],
        compiler_params=pltpu.CompilerParams(vmem_limit_bytes=FINISH_MIB * 1024 * 1024),
    )(offsets, stats, solution, direction_in, back_image, back_residual, images, residual_in)
    return results[0], results[1].reshape(residual.shape), results[2], results[3]


def solution(mesh):
    placed = (
        P(("scan", "slab"), None),
        P(("scan", "slab"), None),
        P(("scan", "slab"), None),
        P(("scan", "slab"), None, None),
        P(),
        P(("scan", "slab")),
    )
    return jax.shard_map(
        functools.partial(local, mesh.shape["slab"]),
        mesh=mesh,
        in_specs=placed,
        out_specs=(
            P(("scan", "slab"), None),
            P(("scan", "slab"), None, None),
            P(("scan", "slab"), None),
            P(("scan", "slab"), None),
        ),
        check_vma=False,
    )
```

```python
import functools

import jax
import jax.numpy as jnp
from jax import lax
from jax.experimental import pallas as pl
from jax.experimental.pallas import tpu as pltpu
from jax.sharding import PartitionSpec as P

LANES = 128
STATS = 5
PROJECT_MIB = 30
FINISH_MIB = 8


def split(value):
    upper = value.astype(jnp.bfloat16)
    return upper, (value - upper.astype(jnp.float32)).astype(jnp.bfloat16)


def fold_tile(value):
    total = None
    for r in range(0, value.shape[0], 8):
        for c in range(0, value.shape[1], LANES):
            tile = value[r : r + 8, c : c + LANES]
            total = tile if total is None else total + tile
    return total


def project(
    count,
    offsets_hbm,
    direction_hbm,
    gradient_hbm,
    residual_hbm,
    tiles_hbm,
    residual_vm,
    windows,
    direction_vm,
    back_image,
    back_residual,
    stats_out,
    offsets_sm,
    gradient_vm,
    tiles_vm,
    own,
    halo,
    images,
    hits,
    covers,
    covers_in,
    times,
    image_sums,
    sums_own,
    sums_out,
    sums_in,
    stacked,
    partial,
    stat_send,
    stat_recv,
    load_sems,
    residual_sems,
    tile_sems,
    side_send,
    cover_recv,
    sums_send,
    sums_recv,
    halo_recv,
    stat_sems,
):
    scope = jax.named_scope
    me = lax.axis_index("slab")
    planes, cells = direction_vm.shape
    per_angle, angles, rows, columns = residual_vm.shape
    near = 3 * planes
    half = angles // 2
    pairs = (range(0, half), range(half, angles))
    last = angles - 1
    f32, bf16 = jnp.float32, jnp.bfloat16
    has_low = me > 0
    has_high = me < count - 1
    late = me >= count - count // 4
    early = me < count // 2
    low = {"slab": lax.rem(me + count - 1, count)}
    high = {"slab": lax.rem(me + 1, count)}

    load_offsets = pltpu.make_async_copy(offsets_hbm, offsets_sm, load_sems.at[0])
    load_direction = pltpu.make_async_copy(direction_hbm, direction_vm, load_sems.at[1])
    load_gradient = pltpu.make_async_copy(gradient_hbm, gradient_vm, load_sems.at[0])

    groups = [(a, 1) for a in pairs[0]] + [(half, angles - half)]

    def load_residual(group):
        angles_of = pl.ds(*groups[group])
        return pltpu.make_async_copy(
            residual_hbm.at[:, angles_of], residual_vm.at[:, angles_of], residual_sems.at[group]
        )

    def load_tile(a):
        sem = residual_sems.at[0] if a == last else tile_sems.at[a]
        return pltpu.make_async_copy(tiles_hbm.at[a], tiles_vm.at[a], sem)

    load_offsets.start()
    for group in range(len(groups)):
        load_residual(group).start()
    load_direction.start()
    for a in range(last):
        load_tile(a).start(priority=1)

    barrier = pltpu.get_barrier_semaphore()
    for d in range(1, count):
        pl.semaphore_signal(barrier, inc=1, device_id={"slab": lax.rem(me + d, count)})

    @pl.when(jnp.logical_not(has_low))
    def _():
        halo[:planes, :] = jnp.zeros((planes, cells), bf16)
        covers_in[0] = jnp.zeros((planes, LANES), bf16)
        sums_in[0] = jnp.zeros((angles, planes, columns), bf16)

    @pl.when(jnp.logical_not(has_high))
    def _():
        halo[planes:, :] = jnp.zeros((planes, cells), bf16)
        covers_in[1] = jnp.zeros((planes, LANES), bf16)
        sums_in[1] = jnp.zeros((angles, planes, columns), bf16)

    with scope("w_off"):
        load_offsets.wait()
    shift = planes - me * planes

    lane = lax.broadcasted_iota(jnp.int32, (near, LANES), 1)
    plane = lax.broadcasted_iota(jnp.int32, (near, LANES), 0)
    first = jnp.full((near, LANES), near, jnp.int32)
    for v in range(angles * per_angle):
        first = jnp.where(lane == v, offsets_sm[v] + shift, first)
    inside = jnp.logical_and(plane >= first, plane < first + rows)
    covers[...] = jnp.where(inside, 1.0, 0.0).astype(bf16)

    plane_id = lax.broadcasted_iota(jnp.int32, (near, per_angle * rows), 0)
    row_id = lax.broadcasted_iota(jnp.int32, (near, per_angle * rows), 1)
    for a in range(angles):
        base = jnp.zeros_like(row_id)
        for j in range(per_angle):
            base = jnp.where(row_id >= j * rows, offsets_sm[j * angles + a] + shift - j * rows, base)
        hits[a] = jnp.where(plane_id == row_id + base, 1.0, 0.0).astype(bf16)

    def cover_copy(side):
        source = covers.at[pl.ds(0 if side == 0 else 2 * planes, planes)]
        return pltpu.make_async_remote_copy(
            source, covers_in.at[1 - side], side_send.at[side], cover_recv.at[1 - side],
            device_id=low if side == 0 else high,
        )

    def sums_copy(side, group):
        angles_of = pl.ds(*groups[group])
        return pltpu.make_async_remote_copy(
            sums_out.at[side, angles_of], sums_in.at[1 - side, angles_of],
            sums_send.at[side], sums_recv.at[1 - side, group // half],
            device_id=low if side == 0 else high,
        )

    def sums_wait(side, pair):
        landed = sums_in.at[side, pl.ds(pairs[pair][0], len(pairs[pair]))]
        pltpu.make_async_copy(landed, landed, sums_recv.at[side, pair]).wait()

    def sums_sent(side):
        pltpu.make_async_copy(sums_out.at[side], sums_out.at[side], sums_send.at[side]).wait()

    def halo_copy(side):
        return pltpu.make_async_remote_copy(
            own, halo.at[pl.ds((1 - side) * planes, planes)], side_send.at[side], halo_recv.at[1 - side],
            device_id=low if side == 0 else high,
        )

    def each_side(action):
        @pl.when(has_low)
        def _():
            action(0)

        @pl.when(has_high)
        def _():
            action(1)

    for group, (start, size) in enumerate(groups):
        with scope("w_res"):
            load_residual(group).wait()
        for a in range(start, start + size):
            upper, lower = split(residual_vm[:, a].reshape(per_angle * rows, columns))
            sums = jnp.dot(hits[a], upper, preferred_element_type=f32) + jnp.dot(
                hits[a], lower, preferred_element_type=f32
            )
            sums_own[a] = sums[planes : 2 * planes]
            sums_out[0, a] = sums[:planes].astype(bf16)
            sums_out[1, a] = sums[2 * planes :].astype(bf16)
        if group == 0:
            with scope("w_bar"):
                pl.semaphore_wait(barrier, count - 1)
            each_side(lambda side: cover_copy(side).start())
        each_side(lambda side: sums_copy(side, group).start())

    load_tile(last).start(priority=1)
    with scope("w_dir"):
        load_direction.wait()
    own[...] = direction_vm[...].astype(bf16)

    view_of = lax.broadcasted_iota(jnp.int32, (LANES, angles * LANES), 0)
    lane_of = lax.broadcasted_iota(jnp.int32, (LANES, angles * LANES), 1)
    chosen = jnp.where(lax.rem(view_of, angles) == lane_of // LANES, 1.0, 0.0).astype(bf16)
    product_sums = [jnp.zeros((8, LANES), f32)] * 3

    def backward(first_angle, last_angle):
        chunk = 2 * LANES
        for p in range(0, cells, chunk):
            part = None
            for a in range(first_angle, last_angle):
                product = lax.dot_general(
                    tiles_vm[a, p : p + chunk], stacked[a], (((1,), (1,)), ((), ())), preferred_element_type=f32
                )
                part = product if part is None else part + product
            if first_angle > 0:
                part = part + partial[p : p + chunk]
            if last_angle < angles:
                partial[p : p + chunk] = part
                continue
            turned = part.T
            from_image, from_residual = turned[:planes], turned[planes:]
            back_image[:, p : p + chunk] = from_image
            back_residual[:, p : p + chunk] = from_residual
            product_sums[0] = product_sums[0] + fold_tile(from_residual * from_residual)
            product_sums[1] = product_sums[1] + fold_tile(from_residual * from_image)
            product_sums[2] = product_sums[2] + fold_tile(from_image * from_image)

    def forward(a):
        image = jnp.dot(own[...], tiles_vm[a], preferred_element_type=f32)
        for l in range(columns // LANES):
            images[a, l, planes : 2 * planes] = image[:, l * LANES : (l + 1) * LANES]

    def count_covers():
        covered = covers[planes : 2 * planes].astype(f32) + covers_in[0].astype(f32) + covers_in[1].astype(f32)
        times[...] = jnp.dot(covered.astype(bf16), chosen, preferred_element_type=f32)

    def weigh(a):
        squares = None
        for l in range(columns // LANES):
            piece = images[a, l, planes : 2 * planes]
            weighted = times[:, a * LANES : (a + 1) * LANES] * piece
            stacked[a, :planes, l * LANES : (l + 1) * LANES] = weighted.astype(bf16)
            square = fold_tile(weighted * piece)
            squares = square if squares is None else squares + square
        image_sums[a] = squares

    def wait_tile(a):
        with scope("w_tile"):
            load_tile(a).wait()

    for a in pairs[0]:
        wait_tile(a)
        forward(a)
    with scope("w_cov"):
        each_side(lambda side: cover_copy(side).wait_send())
        each_side(lambda side: cover_copy(1 - side).wait_recv())
    each_side(lambda side: halo_copy(side).start())

    @pl.when(jnp.logical_not(late))
    def _():
        for a in range(half, last):
            wait_tile(a)
            if a == half:
                count_covers()
                weigh(0)
            forward(a)
        for a in range(1, last):
            weigh(a)

    @pl.when(early)
    def _():
        wait_tile(last)
        forward(last)
        weigh(last)

    @pl.when(late)
    def _():
        count_covers()
        for a in pairs[0]:
            weigh(a)

    def stack(pair):
        with scope("w_sums"):
            each_side(lambda side: sums_wait(side, pair))
        for a in pairs[pair]:
            sums = sums_own[a] + sums_in[0, a].astype(f32) + sums_in[1, a].astype(f32)
            stacked[a, planes:] = sums.astype(bf16)

    stack(0)
    load_gradient.start(priority=1)
    with scope("bwd"):
        backward(0, half)

    @pl.when(late)
    def _():
        for a in pairs[1]:
            wait_tile(a)
        for a in pairs[1]:
            forward(a)
        for a in pairs[1]:
            weigh(a)

    @pl.when(jnp.logical_not(jnp.logical_or(early, late)))
    def _():
        wait_tile(last)
        forward(last)
        weigh(last)

    with scope("w_grad"):
        load_gradient.wait()
    stack(1)
    with scope("bwd"):
        gradient_sums = fold_tile(gradient_vm[...] * gradient_vm[...])
        backward(half, angles)

    image_total = image_sums[0]
    for a in range(1, angles):
        image_total = image_total + image_sums[a]
    stat_send[...] = jnp.concatenate(
        [jnp.sum(x, axis=0, keepdims=True) for x in [gradient_sums, image_total] + product_sums]
        + [jnp.zeros((8 - STATS, LANES), f32)],
        axis=0,
    )
    for d in range(1, count):
        pltpu.make_async_remote_copy(
            stat_send, stat_recv.at[d - 1], stat_sems.at[0], stat_sems.at[1],
            device_id={"slab": lax.rem(me + d, count)},
        ).start()

    with scope("w_halo"):
        each_side(lambda side: halo_copy(side).wait_send())
        each_side(lambda side: halo_copy(1 - side).wait_recv())

    with scope("fwdhalo"):
        for a in range(angles):
            image = jnp.dot(halo[...], tiles_vm[a], preferred_element_type=f32)
            for l in range(columns // LANES):
                cut = slice(l * LANES, (l + 1) * LANES)
                images[a, l, :planes] = image[:planes, cut]
                images[a, l, 2 * planes :] = image[planes:, cut]

    with scope("windows"):
        for j in range(per_angle):
            for a in range(angles):
                top = jnp.clip(offsets_sm[j * angles + a] + shift, 0, near - rows)
                for l in range(columns // LANES):
                    windows[j, a, :, l * LANES : (l + 1) * LANES] = images[a, l, pl.ds(top, rows), :]

    each_side(sums_sent)
    with scope("w_stat"):
        pltpu.make_async_copy(stat_recv, stat_recv, stat_sems.at[0]).wait()
        pltpu.make_async_copy(stat_recv, stat_recv, stat_sems.at[1]).wait()
    sums = stat_send[...]
    for d in range(1, count):
        sums = sums + stat_recv[d - 1]
    norms = jnp.sum(sums, axis=1, keepdims=True)
    grad_norm, image_norm = norms[0:1], norms[1:2]
    step_size = grad_norm / image_norm
    new_norm = norms[2:3] - 2.0 * step_size * norms[3:4] + step_size * step_size * norms[4:5]
    stats_out[...] = jnp.concatenate(
        [
            jnp.broadcast_to(step_size, (1, LANES)),
            jnp.broadcast_to(new_norm / grad_norm, (1, LANES)),
            jnp.zeros((6, LANES), f32),
        ],
        axis=0,
    )


def finish(
    stats, solution_ref, direction_ref, back_image, back_residual, windows, residual_ref,
    solution_out, residual_out, gradient_out, direction_out,
    volumes_vm, residual_vm, sems,
):
    per_angle, angles = residual_ref.shape[:2]
    step_size = stats[0:1, 0:1]
    scale = stats[1:2, 0:1]
    for j in range(per_angle):
        for a in range(angles):
            residual_vm[j, a] = residual_ref[j, a] - step_size * windows[j, a]
            pltpu.make_async_copy(residual_vm.at[j, a], residual_out.at[j, a], sems.at[0]).start()
    gradient = back_residual[...] - step_size * back_image[...]
    volumes_vm[0] = gradient
    pltpu.make_async_copy(volumes_vm.at[0], gradient_out, sems.at[1]).start()
    volumes_vm[1] = gradient + scale * direction_ref[...]
    pltpu.make_async_copy(volumes_vm.at[1], direction_out, sems.at[1]).start()
    volumes_vm[2] = solution_ref[...] + step_size * direction_ref[...]
    pltpu.make_async_copy(volumes_vm.at[2], solution_out, sems.at[1]).start()
    pltpu.make_async_copy(residual_vm, residual_out, sems.at[0]).wait()
    pltpu.make_async_copy(volumes_vm, volumes_vm, sems.at[1]).wait()


def local(count, solution, direction, gradient, residual, tiles, offsets):
    planes, cells = solution.shape
    views, rows, columns = residual.shape
    angles = tiles.shape[0]
    per_angle = views // angles
    near = 3 * planes
    half = angles // 2
    f32, bf16 = jnp.float32, jnp.bfloat16
    hbm = pl.BlockSpec(memory_space=pltpu.HBM)
    vmem = pl.BlockSpec(memory_space=pltpu.VMEM)
    dma = pltpu.SemaphoreType.DMA
    by_angle = residual.reshape(per_angle, angles, rows, columns)
    volume = jax.ShapeDtypeStruct((planes, cells), f32)
    detector = jax.ShapeDtypeStruct(by_angle.shape, f32)
    remote = [pltpu.with_memory_space_constraint(x, pltpu.HBM) for x in (offsets, direction, gradient, by_angle, tiles)]
    residual_in, windows, direction_in, back_image, back_residual, stats = pl.pallas_call(
        functools.partial(project, count),
        name="project",
        out_shape=(detector, detector, volume, volume, volume, jax.ShapeDtypeStruct((8, LANES), f32)),
        in_specs=[hbm] * 5,
        out_specs=(vmem,) * 6,
        scratch_shapes=[
            pltpu.SMEM((views,), jnp.int32),
            pltpu.VMEM((planes, cells), f32),
            pltpu.VMEM((angles, cells, columns), bf16),
            pltpu.VMEM((planes, cells), bf16),
            pltpu.VMEM((2 * planes, cells), bf16),
            pltpu.VMEM((angles, columns // LANES, near, LANES), f32),
            pltpu.VMEM((angles, near, per_angle * rows), bf16),
            pltpu.VMEM((near, LANES), bf16),
            pltpu.VMEM((2, planes, LANES), bf16),
            pltpu.VMEM((planes, angles * LANES), f32),
            pltpu.VMEM((angles, 8, LANES), f32),
            pltpu.VMEM((angles, planes, columns), f32),
            pltpu.VMEM((2, angles, planes, columns), bf16),
            pltpu.VMEM((2, angles, planes, columns), bf16),
            pltpu.VMEM((angles, 2 * planes, columns), bf16),
            pltpu.VMEM((cells, 2 * planes), f32),
            pltpu.VMEM((8, LANES), f32),
            pltpu.VMEM((count - 1, 8, LANES), f32),
            dma((2,)),
            dma((half + 1,)),
            dma((angles - 1,)),
            dma((2,)),
            dma((2,)),
            dma((2,)),
            dma((2, 2)),
            dma((2,)),
            dma((2,)),
        ],
        compiler_params=pltpu.CompilerParams(
            collective_id=0, has_side_effects=True, vmem_limit_bytes=PROJECT_MIB * 1024 * 1024
        ),
    )(*remote)
    results = pl.pallas_call(
        finish,
        name="finish",
        out_shape=(volume, detector, volume, volume),
        in_specs=[vmem] * 7,
        out_specs=(hbm,) * 4,
        scratch_shapes=[
            pltpu.VMEM((3, planes, cells), f32),
            pltpu.VMEM(by_angle.shape, f32),
            dma((2,)),
        ],
        compiler_params=pltpu.CompilerParams(vmem_limit_bytes=FINISH_MIB * 1024 * 1024),
    )(stats, solution, direction_in, back_image, back_residual, windows, residual_in)
    return results[0], results[1].reshape(residual.shape), results[2], results[3]


def solution(mesh):
    placed = (
        P(("scan", "slab"), None),
        P(("scan", "slab"), None),
        P(("scan", "slab"), None),
        P(("scan", "slab"), None, None),
        P(),
        P(("scan", "slab")),
    )
    return jax.shard_map(
        functools.partial(local, mesh.shape["slab"]),
        mesh=mesh,
        in_specs=placed,
        out_specs=(
            P(("scan", "slab"), None),
            P(("scan", "slab"), None, None),
            P(("scan", "slab"), None),
            P(("scan", "slab"), None),
        ),
        check_vma=False,
    )
```

```python
import functools

import jax
import jax.numpy as jnp
from jax import lax
from jax.experimental import pallas as pl
from jax.experimental.pallas import tpu as pltpu
from jax.sharding import PartitionSpec as P

LANES = 128
STATS = 5
PROJECT_MIB = 30
FINISH_MIB = 8


def split(value):
    upper = value.astype(jnp.bfloat16)
    return upper, (value - upper.astype(jnp.float32)).astype(jnp.bfloat16)


def fold_tile(value):
    total = None
    for r in range(0, value.shape[0], 8):
        for c in range(0, value.shape[1], LANES):
            tile = value[r : r + 8, c : c + LANES]
            total = tile if total is None else total + tile
    return total


def project(
    count,
    offsets_hbm,
    direction_hbm,
    gradient_hbm,
    residual_hbm,
    tiles_hbm,
    residual_vm,
    windows,
    direction_vm,
    back_image,
    back_residual,
    stats_out,
    offsets_sm,
    gradient_vm,
    tiles_vm,
    own,
    halo,
    images,
    hits,
    covers,
    covers_in,
    times,
    image_sums,
    product_sums,
    gradient_sums,
    sums_own,
    sums_out,
    sums_in,
    stacked,
    partial,
    stat_send,
    stat_recv,
    load_sems,
    residual_sems,
    tile_sems,
    side_send,
    cover_recv,
    sums_send,
    sums_recv,
    halo_recv,
    stat_sems,
):
    scope = jax.named_scope
    me = lax.axis_index("slab")
    planes, cells = direction_vm.shape
    per_angle, angles, rows, columns = residual_vm.shape
    near = 3 * planes
    half = angles // 2
    pairs = (range(0, half), range(half, angles))
    last = angles - 1
    f32, bf16 = jnp.float32, jnp.bfloat16
    has_low = me > 0
    has_high = me < count - 1
    late = me >= count - count // 4
    early = me < count // 2
    low = {"slab": lax.rem(me + count - 1, count)}
    high = {"slab": lax.rem(me + 1, count)}

    load_offsets = pltpu.make_async_copy(offsets_hbm, offsets_sm, load_sems.at[0])
    load_direction = pltpu.make_async_copy(direction_hbm, direction_vm, load_sems.at[1])
    load_gradient = pltpu.make_async_copy(gradient_hbm, gradient_vm, load_sems.at[0])

    groups = [(a, 1) for a in pairs[0]] + [(half, angles - half)]

    def load_residual(group):
        angles_of = pl.ds(*groups[group])
        return pltpu.make_async_copy(
            residual_hbm.at[:, angles_of], residual_vm.at[:, angles_of], residual_sems.at[group]
        )

    middle = cells // 2
    pieces = {a: ((0, cells),) if a in (0, last) else ((0, middle), (middle, cells - middle)) for a in range(angles)}

    def load_tile(a, part):
        cut = pl.ds(*pieces[a][part])
        sem = residual_sems.at[0] if a == last else tile_sems.at[2 * a + part]
        return pltpu.make_async_copy(tiles_hbm.at[a, cut], tiles_vm.at[a, cut], sem)

    load_offsets.start()
    for group in range(len(groups)):
        load_residual(group).start()
    load_direction.start()
    for a in range(last):
        for part in range(len(pieces[a])):
            load_tile(a, part).start(priority=1)

    barrier = pltpu.get_barrier_semaphore()
    for d in range(1, count):
        pl.semaphore_signal(barrier, inc=1, device_id={"slab": lax.rem(me + d, count)})

    @pl.when(jnp.logical_not(has_low))
    def _():
        halo[:planes, :] = jnp.zeros((planes, cells), bf16)
        covers_in[0] = jnp.zeros((planes, LANES), bf16)
        sums_in[0] = jnp.zeros((angles, planes, columns), bf16)

    @pl.when(jnp.logical_not(has_high))
    def _():
        halo[planes:, :] = jnp.zeros((planes, cells), bf16)
        covers_in[1] = jnp.zeros((planes, LANES), bf16)
        sums_in[1] = jnp.zeros((angles, planes, columns), bf16)

    with scope("w_off"):
        load_offsets.wait()
    shift = planes - me * planes

    lane = lax.broadcasted_iota(jnp.int32, (near, LANES), 1)
    plane = lax.broadcasted_iota(jnp.int32, (near, LANES), 0)
    first = jnp.full((near, LANES), near, jnp.int32)
    for v in range(angles * per_angle):
        first = jnp.where(lane == v, offsets_sm[v] + shift, first)
    inside = jnp.logical_and(plane >= first, plane < first + rows)
    covers[...] = jnp.where(inside, 1.0, 0.0).astype(bf16)

    plane_id = lax.broadcasted_iota(jnp.int32, (near, per_angle * rows), 0)
    row_id = lax.broadcasted_iota(jnp.int32, (near, per_angle * rows), 1)
    for a in range(angles):
        base = jnp.zeros_like(row_id)
        for j in range(per_angle):
            base = jnp.where(row_id >= j * rows, offsets_sm[j * angles + a] + shift - j * rows, base)
        hits[a] = jnp.where(plane_id == row_id + base, 1.0, 0.0).astype(bf16)

    def cover_copy(side):
        source = covers.at[pl.ds(0 if side == 0 else 2 * planes, planes)]
        return pltpu.make_async_remote_copy(
            source, covers_in.at[1 - side], side_send.at[side], cover_recv.at[1 - side],
            device_id=low if side == 0 else high,
        )

    def sums_copy(side, group):
        angles_of = pl.ds(*groups[group])
        return pltpu.make_async_remote_copy(
            sums_out.at[side, angles_of], sums_in.at[1 - side, angles_of],
            sums_send.at[side], sums_recv.at[1 - side, group],
            device_id=low if side == 0 else high,
        )

    def sums_sent(side):
        pltpu.make_async_copy(sums_out.at[side], sums_out.at[side], sums_send.at[side]).wait()

    def halo_copy(side):
        return pltpu.make_async_remote_copy(
            own, halo.at[pl.ds((1 - side) * planes, planes)], side_send.at[side], halo_recv.at[1 - side],
            device_id=low if side == 0 else high,
        )

    def each_side(action):
        @pl.when(has_low)
        def _():
            action(0)

        @pl.when(has_high)
        def _():
            action(1)

    for group, (start, size) in enumerate(groups):
        with scope("w_res"):
            load_residual(group).wait()
        if group == 0:
            load_tile(last, 0).start(priority=1)
        for a in range(start, start + size):
            upper, lower = split(residual_vm[:, a].reshape(per_angle * rows, columns))
            sums = jnp.dot(hits[a], upper, preferred_element_type=f32) + jnp.dot(
                hits[a], lower, preferred_element_type=f32
            )
            sums_own[a] = sums[planes : 2 * planes]
            sums_out[0, a] = sums[:planes].astype(bf16)
            sums_out[1, a] = sums[2 * planes :].astype(bf16)
        if group == 0:
            with scope("w_bar"):
                pl.semaphore_wait(barrier, count - 1)
            each_side(lambda side: cover_copy(side).start())
        each_side(lambda side: sums_copy(side, group).start())

    with scope("w_dir"):
        load_direction.wait()
    own[...] = direction_vm[...].astype(bf16)

    view_of = lax.broadcasted_iota(jnp.int32, (LANES, angles * LANES), 0)
    lane_of = lax.broadcasted_iota(jnp.int32, (LANES, angles * LANES), 1)
    chosen = jnp.where(lax.rem(view_of, angles) == lane_of // LANES, 1.0, 0.0).astype(bf16)

    def backward(first_angle, last_angle):
        chunk = 2 * LANES
        squares = [None] * 3
        for p in range(0, cells, chunk):
            part = None
            for a in range(first_angle, last_angle):
                product = lax.dot_general(
                    tiles_vm[a, p : p + chunk], stacked[a], (((1,), (1,)), ((), ())), preferred_element_type=f32
                )
                part = product if part is None else part + product
            if first_angle > 0:
                part = part + partial[p : p + chunk]
            if last_angle < angles:
                partial[p : p + chunk] = part
                continue
            turned = part.T
            from_image, from_residual = turned[:planes], turned[planes:]
            back_image[:, p : p + chunk] = from_image
            back_residual[:, p : p + chunk] = from_residual
            for k, (x, y) in enumerate(((from_residual, from_residual), (from_residual, from_image), (from_image, from_image))):
                square = fold_tile(x * y)
                squares[k] = square if squares[k] is None else squares[k] + square
        if last_angle == angles:
            for k in range(3):
                product_sums[k] = squares[k]

    def forward(a, start=0, size=cells):
        cut = pl.ds(start, size)
        image = jnp.dot(own[:, cut], tiles_vm[a, cut], preferred_element_type=f32)
        for l in range(columns // LANES):
            piece = image[:, l * LANES : (l + 1) * LANES]
            if start > 0:
                piece = piece + images[a, l, planes : 2 * planes]
            images[a, l, planes : 2 * planes] = piece

    def count_covers():
        covered = covers[planes : 2 * planes].astype(f32) + covers_in[0].astype(f32) + covers_in[1].astype(f32)
        times[...] = jnp.dot(covered.astype(bf16), chosen, preferred_element_type=f32)

    def weigh(a):
        squares = None
        for l in range(columns // LANES):
            piece = images[a, l, planes : 2 * planes]
            weighted = times[:, a * LANES : (a + 1) * LANES] * piece
            stacked[a, :planes, l * LANES : (l + 1) * LANES] = weighted.astype(bf16)
            square = fold_tile(weighted * piece)
            squares = square if squares is None else squares + square
        image_sums[a] = squares

    def wait_part(a, part):
        with scope("w_tile"):
            load_tile(a, part).wait()

    def wait_tile(a):
        for part in range(len(pieces[a])):
            wait_part(a, part)

    def forward_parts(a, before=()):
        for part, (start, size) in enumerate(pieces[a]):
            wait_part(a, part)
            if part == 0:
                for action in before:
                    action()
            forward(a, start, size)

    def take_covers():
        with scope("w_cov"):
            each_side(lambda side: cover_copy(side).wait_send())
            each_side(lambda side: cover_copy(1 - side).wait_recv())
        each_side(lambda side: halo_copy(side).start())

    def wait_sums(start, stop):
        for group, (first_angle, size) in enumerate(groups):
            if start <= first_angle < stop:
                with scope("w_sums"):
                    each_side(lambda side: sums_copy(1 - side, group).wait_recv())

    def stack(start, stop):
        for a in range(start, stop):
            sums = sums_own[a] + sums_in[0, a].astype(f32) + sums_in[1, a].astype(f32)
            stacked[a, planes:] = sums.astype(bf16)

    def weigh_first():
        count_covers()
        for a in pairs[0]:
            weigh(a)

    def first_pair():
        wait_sums(0, half)
        load_gradient.start(priority=1)
        with scope("bwd"):
            stack(0, half)
            backward(0, half)

    def second_pair(angles_left):
        for a in angles_left:
            wait_tile(a)
        with scope("w_grad"):
            load_gradient.wait()
        wait_sums(half, angles)
        with scope("bwd2"):
            gradient_sums[...] = fold_tile(gradient_vm[...] * gradient_vm[...])
            stack(half, angles)
            for a in angles_left:
                forward(a)
            for a in angles_left:
                weigh(a)
            backward(half, angles)
            image_total = image_sums[0]
            for a in range(1, angles):
                image_total = image_total + image_sums[a]
            parts = (gradient_sums[...], image_total, product_sums[0], product_sums[1], product_sums[2])
            stat_send[...] = jnp.concatenate([jnp.sum(x, axis=0, keepdims=True) for x in parts], axis=0)
        for d in range(1, count):
            pltpu.make_async_remote_copy(
                stat_send, stat_recv.at[d - 1], stat_sems.at[0], stat_sems.at[1],
                device_id={"slab": lax.rem(me + d, count)},
            ).start()

    @pl.when(late)
    def _():
        wait_tile(0)
        forward(0)
        take_covers()
        for a in range(1, half):
            forward_parts(a, (count_covers, functools.partial(weigh, 0)) if a == 1 else ())
            weigh(a)
        first_pair()
        second_pair(range(half, angles))

    @pl.when(jnp.logical_not(jnp.logical_or(early, late)))
    def _():
        for a in pairs[0]:
            forward_parts(a)
        take_covers()
        for a in range(half, last):
            forward_parts(a, (weigh_first,) if a == half else ())
            weigh(a)
        first_pair()
        second_pair(range(last, angles))

    @pl.when(early)
    def _():
        for a in pairs[0]:
            wait_tile(a)
            forward(a)
        take_covers()
        for a in range(half, angles):
            wait_tile(a)
            if a == half:
                weigh_first()
            forward(a)
            weigh(a)
        first_pair()
        second_pair(())

    with scope("w_halo"):
        each_side(lambda side: halo_copy(side).wait_send())
        each_side(lambda side: halo_copy(1 - side).wait_recv())

    with scope("fwdhalo"):
        for a in range(angles):
            image = jnp.dot(halo[...], tiles_vm[a], preferred_element_type=f32)
            for l in range(columns // LANES):
                cut = slice(l * LANES, (l + 1) * LANES)
                images[a, l, :planes] = image[:planes, cut]
                images[a, l, 2 * planes :] = image[planes:, cut]

    with scope("windows"):
        for j in range(per_angle):
            for a in range(angles):
                top = jnp.clip(offsets_sm[j * angles + a] + shift, 0, near - rows)
                for l in range(columns // LANES):
                    windows[j, a, :, l * LANES : (l + 1) * LANES] = images[a, l, pl.ds(top, rows), :]

    each_side(sums_sent)
    with scope("w_stat"):
        pltpu.make_async_copy(stat_recv, stat_recv, stat_sems.at[0]).wait()
        pltpu.make_async_copy(stat_recv, stat_recv, stat_sems.at[1]).wait()
    sums = stat_send[...]
    for d in range(1, count):
        sums = sums + stat_recv[d - 1]
    norms = jnp.sum(sums, axis=1, keepdims=True)
    grad_norm, image_norm = norms[0:1], norms[1:2]
    step_size = grad_norm / image_norm
    new_norm = norms[2:3] - 2.0 * step_size * norms[3:4] + step_size * step_size * norms[4:5]
    stats_out[...] = jnp.concatenate(
        [
            jnp.broadcast_to(step_size, (1, LANES)),
            jnp.broadcast_to(new_norm / grad_norm, (1, LANES)),
            jnp.zeros((6, LANES), f32),
        ],
        axis=0,
    )


def finish(
    stats, solution_ref, direction_ref, back_image, back_residual, windows, residual_ref,
    solution_out, residual_out, gradient_out, direction_out,
    volumes_vm, residual_vm, sems,
):
    per_angle, angles = residual_ref.shape[:2]
    step_size = stats[0:1, 0:1]
    scale = stats[1:2, 0:1]
    for j in range(per_angle):
        for a in range(angles):
            residual_vm[j, a] = residual_ref[j, a] - step_size * windows[j, a]
            pltpu.make_async_copy(residual_vm.at[j, a], residual_out.at[j, a], sems.at[0]).start()
    gradient = back_residual[...] - step_size * back_image[...]
    volumes_vm[0] = gradient
    pltpu.make_async_copy(volumes_vm.at[0], gradient_out, sems.at[1]).start()
    volumes_vm[1] = gradient + scale * direction_ref[...]
    pltpu.make_async_copy(volumes_vm.at[1], direction_out, sems.at[1]).start()
    volumes_vm[2] = solution_ref[...] + step_size * direction_ref[...]
    pltpu.make_async_copy(volumes_vm.at[2], solution_out, sems.at[1]).start()
    pltpu.make_async_copy(residual_vm, residual_out, sems.at[0]).wait()
    pltpu.make_async_copy(volumes_vm, volumes_vm, sems.at[1]).wait()


def local(count, solution, direction, gradient, residual, tiles, offsets):
    planes, cells = solution.shape
    views, rows, columns = residual.shape
    angles = tiles.shape[0]
    per_angle = views // angles
    near = 3 * planes
    half = angles // 2
    f32, bf16 = jnp.float32, jnp.bfloat16
    hbm = pl.BlockSpec(memory_space=pltpu.HBM)
    vmem = pl.BlockSpec(memory_space=pltpu.VMEM)
    dma = pltpu.SemaphoreType.DMA
    by_angle = residual.reshape(per_angle, angles, rows, columns)
    volume = jax.ShapeDtypeStruct((planes, cells), f32)
    detector = jax.ShapeDtypeStruct(by_angle.shape, f32)
    remote = [pltpu.with_memory_space_constraint(x, pltpu.HBM) for x in (offsets, direction, gradient, by_angle, tiles)]
    residual_in, windows, direction_in, back_image, back_residual, stats = pl.pallas_call(
        functools.partial(project, count),
        name="project",
        out_shape=(detector, detector, volume, volume, volume, jax.ShapeDtypeStruct((8, LANES), f32)),
        in_specs=[hbm] * 5,
        out_specs=(vmem,) * 6,
        scratch_shapes=[
            pltpu.SMEM((views,), jnp.int32),
            pltpu.VMEM((planes, cells), f32),
            pltpu.VMEM((angles, cells, columns), bf16),
            pltpu.VMEM((planes, cells), bf16),
            pltpu.VMEM((2 * planes, cells), bf16),
            pltpu.VMEM((angles, columns // LANES, near, LANES), f32),
            pltpu.VMEM((angles, near, per_angle * rows), bf16),
            pltpu.VMEM((near, LANES), bf16),
            pltpu.VMEM((2, planes, LANES), bf16),
            pltpu.VMEM((planes, angles * LANES), f32),
            pltpu.VMEM((angles, 8, LANES), f32),
            pltpu.VMEM((3, 8, LANES), f32),
            pltpu.VMEM((8, LANES), f32),
            pltpu.VMEM((angles, planes, columns), f32),
            pltpu.VMEM((2, angles, planes, columns), bf16),
            pltpu.VMEM((2, angles, planes, columns), bf16),
            pltpu.VMEM((angles, 2 * planes, columns), bf16),
            pltpu.VMEM((cells, 2 * planes), f32),
            pltpu.VMEM((STATS, LANES), f32),
            pltpu.VMEM((count - 1, STATS, LANES), f32),
            dma((2,)),
            dma((half + 1,)),
            dma((2 * angles - 2,)),
            dma((2,)),
            dma((2,)),
            dma((2,)),
            dma((2, half + 1)),
            dma((2,)),
            dma((2,)),
        ],
        compiler_params=pltpu.CompilerParams(
            collective_id=0, has_side_effects=True, vmem_limit_bytes=PROJECT_MIB * 1024 * 1024
        ),
    )(*remote)
    results = pl.pallas_call(
        finish,
        name="finish",
        out_shape=(volume, detector, volume, volume),
        in_specs=[vmem] * 7,
        out_specs=(hbm,) * 4,
        scratch_shapes=[
            pltpu.VMEM((3, planes, cells), f32),
            pltpu.VMEM(by_angle.shape, f32),
            dma((2,)),
        ],
        compiler_params=pltpu.CompilerParams(vmem_limit_bytes=FINISH_MIB * 1024 * 1024),
    )(stats, solution, direction_in, back_image, back_residual, windows, residual_in)
    return results[0], results[1].reshape(residual.shape), results[2], results[3]


def solution(mesh):
    placed = (
        P(("scan", "slab"), None),
        P(("scan", "slab"), None),
        P(("scan", "slab"), None),
        P(("scan", "slab"), None, None),
        P(),
        P(("scan", "slab")),
    )
    return jax.shard_map(
        functools.partial(local, mesh.shape["slab"]),
        mesh=mesh,
        in_specs=placed,
        out_specs=(
            P(("scan", "slab"), None),
            P(("scan", "slab"), None, None),
            P(("scan", "slab"), None),
            P(("scan", "slab"), None),
        ),
        check_vma=False,
    )
```

```python
import functools

import jax
import jax.numpy as jnp
from jax import lax
from jax.experimental import pallas as pl
from jax.experimental.pallas import tpu as pltpu
from jax.sharding import PartitionSpec as P

LANES = 128
STATS = 5
PROJECT_MIB = 30
FINISH_MIB = 8


def split(value):
    upper = value.astype(jnp.bfloat16)
    return upper, (value - upper.astype(jnp.float32)).astype(jnp.bfloat16)


def fold_tile(value):
    total = None
    for r in range(0, value.shape[0], 8):
        for c in range(0, value.shape[1], LANES):
            tile = value[r : r + 8, c : c + LANES]
            total = tile if total is None else total + tile
    return total


def project(
    count,
    offsets_hbm,
    direction_hbm,
    gradient_hbm,
    residual_hbm,
    tiles_hbm,
    residual_vm,
    windows,
    direction_vm,
    back_image,
    back_residual,
    stats_out,
    offsets_sm,
    gradient_vm,
    tiles_vm,
    own,
    halo,
    images,
    hits,
    covers,
    covers_in,
    times,
    image_sums,
    product_sums,
    gradient_sums,
    sums_own,
    sums_out,
    sums_in,
    stacked,
    partial,
    stat_send,
    stat_recv,
    load_sems,
    residual_sems,
    tile_sems,
    side_send,
    cover_recv,
    sums_send,
    sums_recv,
    halo_recv,
    stat_sems,
):
    scope = jax.named_scope
    me = lax.axis_index("slab")
    planes, cells = direction_vm.shape
    per_angle, angles, rows, columns = residual_vm.shape
    near = 3 * planes
    half = angles // 2
    pairs = (range(0, half), range(half, angles))
    last = angles - 1
    f32, bf16 = jnp.float32, jnp.bfloat16
    has_low = me > 0
    has_high = me < count - 1
    late = me >= count - count // 4
    early = me < count // 2
    low = {"slab": lax.rem(me + count - 1, count)}
    high = {"slab": lax.rem(me + 1, count)}

    load_offsets = pltpu.make_async_copy(offsets_hbm, offsets_sm, load_sems.at[0])
    load_direction = pltpu.make_async_copy(direction_hbm, direction_vm, load_sems.at[1])
    load_gradient = pltpu.make_async_copy(gradient_hbm, gradient_vm, load_sems.at[0])

    groups = [(a, 1) for a in pairs[0]] + [(half, angles - half)]

    def load_residual(group):
        angles_of = pl.ds(*groups[group])
        return pltpu.make_async_copy(
            residual_hbm.at[:, angles_of], residual_vm.at[:, angles_of], residual_sems.at[group]
        )

    middle = cells // 2
    pieces = {a: ((0, cells),) if a in (0, last) else ((0, middle), (middle, cells - middle)) for a in range(angles)}

    def load_tile(a, part):
        cut = pl.ds(*pieces[a][part])
        sem = residual_sems.at[0] if a == last else tile_sems.at[max(2 * a - 1, 0) + part]
        return pltpu.make_async_copy(tiles_hbm.at[a, cut], tiles_vm.at[a, cut], sem)

    load_offsets.start()
    for group in range(len(groups)):
        load_residual(group).start()
    load_direction.start()
    for a in range(last):
        for part in range(len(pieces[a])):
            load_tile(a, part).start(priority=1)

    barrier = pltpu.get_barrier_semaphore()
    for d in range(1, count):
        pl.semaphore_signal(barrier, inc=1, device_id={"slab": lax.rem(me + d, count)})

    @pl.when(jnp.logical_not(has_low))
    def _():
        halo[:planes, :] = jnp.zeros((planes, cells), bf16)
        covers_in[0] = jnp.zeros((planes, LANES), bf16)
        sums_in[0] = jnp.zeros((angles, planes, columns), bf16)

    @pl.when(jnp.logical_not(has_high))
    def _():
        halo[planes:, :] = jnp.zeros((planes, cells), bf16)
        covers_in[1] = jnp.zeros((planes, LANES), bf16)
        sums_in[1] = jnp.zeros((angles, planes, columns), bf16)

    with scope("w_off"):
        load_offsets.wait()
    shift = planes - me * planes

    lane = lax.broadcasted_iota(jnp.int32, (near, LANES), 1)
    plane = lax.broadcasted_iota(jnp.int32, (near, LANES), 0)
    first = jnp.full((near, LANES), near, jnp.int32)
    for v in range(angles * per_angle):
        first = jnp.where(lane == v, offsets_sm[v] + shift, first)
    inside = jnp.logical_and(plane >= first, plane < first + rows)
    covers[...] = jnp.where(inside, 1.0, 0.0).astype(bf16)

    plane_id = lax.broadcasted_iota(jnp.int32, (near, per_angle * rows), 0)
    row_id = lax.broadcasted_iota(jnp.int32, (near, per_angle * rows), 1)
    for a in range(angles):
        base = jnp.zeros_like(row_id)
        for j in range(per_angle):
            base = jnp.where(row_id >= j * rows, offsets_sm[j * angles + a] + shift - j * rows, base)
        hits[a] = jnp.where(plane_id == row_id + base, 1.0, 0.0).astype(bf16)

    def cover_copy(side):
        source = covers.at[pl.ds(0 if side == 0 else 2 * planes, planes)]
        return pltpu.make_async_remote_copy(
            source, covers_in.at[1 - side], side_send.at[side], cover_recv.at[1 - side],
            device_id=low if side == 0 else high,
        )

    def sums_copy(side, group):
        angles_of = pl.ds(*groups[group])
        return pltpu.make_async_remote_copy(
            sums_out.at[side, angles_of], sums_in.at[1 - side, angles_of],
            sums_send.at[side], sums_recv.at[1 - side, group // half],
            device_id=low if side == 0 else high,
        )

    def sums_sent(side):
        pltpu.make_async_copy(sums_out.at[side], sums_out.at[side], sums_send.at[side]).wait()

    def halo_copy(side):
        return pltpu.make_async_remote_copy(
            own, halo.at[pl.ds((1 - side) * planes, planes)], side_send.at[side], halo_recv.at[1 - side],
            device_id=low if side == 0 else high,
        )

    def each_side(action):
        @pl.when(has_low)
        def _():
            action(0)

        @pl.when(has_high)
        def _():
            action(1)

    for group, (start, size) in enumerate(groups):
        with scope("w_res"):
            load_residual(group).wait()
        if group == 0:
            load_tile(last, 0).start(priority=1)
        for a in range(start, start + size):
            upper, lower = split(residual_vm[:, a].reshape(per_angle * rows, columns))
            sums = jnp.dot(hits[a], upper, preferred_element_type=f32) + jnp.dot(
                hits[a], lower, preferred_element_type=f32
            )
            sums_own[a] = sums[planes : 2 * planes]
            sums_out[0, a] = sums[:planes].astype(bf16)
            sums_out[1, a] = sums[2 * planes :].astype(bf16)
        if group == 0:
            with scope("w_bar"):
                pl.semaphore_wait(barrier, count - 1)
            each_side(lambda side: cover_copy(side).start())
        each_side(lambda side: sums_copy(side, group).start())

    with scope("w_dir"):
        load_direction.wait()
    own[...] = direction_vm[...].astype(bf16)

    view_of = lax.broadcasted_iota(jnp.int32, (LANES, angles * LANES), 0)
    lane_of = lax.broadcasted_iota(jnp.int32, (LANES, angles * LANES), 1)
    chosen = jnp.where(lax.rem(view_of, angles) == lane_of // LANES, 1.0, 0.0).astype(bf16)

    def backward(first_angle, last_angle):
        chunk = 2 * LANES
        squares = [None] * 3
        cuts = list(range(0, cells, chunk)) + [cells]
        if last_angle == angles:
            cuts.insert(-1, cells - LANES)
        for p, stop in zip(cuts[:-1], cuts[1:]):
            part = None
            for a in range(first_angle, last_angle):
                product = lax.dot_general(
                    tiles_vm[a, p:stop], stacked[a], (((1,), (1,)), ((), ())), preferred_element_type=f32
                )
                part = product if part is None else part + product
            if first_angle > 0:
                part = part + partial[p:stop]
            if last_angle < angles:
                partial[p:stop] = part
                continue
            turned = part.T
            from_image, from_residual = turned[:planes], turned[planes:]
            back_image[:, p:stop] = from_image
            back_residual[:, p:stop] = from_residual
            for k, (x, y) in enumerate(((from_residual, from_residual), (from_residual, from_image), (from_image, from_image))):
                square = fold_tile(x * y)
                squares[k] = square if squares[k] is None else squares[k] + square
        if last_angle == angles:
            for k in range(3):
                product_sums[k] = squares[k]

    def forward(a, start=0, size=cells):
        cut = pl.ds(start, size)
        image = jnp.dot(own[:, cut], tiles_vm[a, cut], preferred_element_type=f32)
        for l in range(columns // LANES):
            piece = image[:, l * LANES : (l + 1) * LANES]
            if start > 0:
                piece = piece + images[a, l, planes : 2 * planes]
            images[a, l, planes : 2 * planes] = piece

    def count_covers():
        covered = covers[planes : 2 * planes].astype(f32) + covers_in[0].astype(f32) + covers_in[1].astype(f32)
        times[...] = jnp.dot(covered.astype(bf16), chosen, preferred_element_type=f32)

    def weigh(a):
        squares = None
        for l in range(columns // LANES):
            piece = images[a, l, planes : 2 * planes]
            weighted = times[:, a * LANES : (a + 1) * LANES] * piece
            stacked[a, :planes, l * LANES : (l + 1) * LANES] = weighted.astype(bf16)
            square = fold_tile(weighted * piece)
            squares = square if squares is None else squares + square
        image_sums[a] = squares

    def wait_part(a, part):
        with scope("w_tile"):
            load_tile(a, part).wait()

    def wait_tile(a):
        for part in range(len(pieces[a])):
            wait_part(a, part)

    def forward_parts(a, before=()):
        for part, (start, size) in enumerate(pieces[a]):
            wait_part(a, part)
            if part == 0:
                for action in before:
                    action()
            forward(a, start, size)

    def take_covers():
        with scope("w_cov"):
            each_side(lambda side: cover_copy(side).wait_send())
            each_side(lambda side: cover_copy(1 - side).wait_recv())
        each_side(lambda side: halo_copy(side).start())

    def sums_wait(side, pair):
        landed = sums_in.at[side, pl.ds(pairs[pair][0], len(pairs[pair]))]
        pltpu.make_async_copy(landed, landed, sums_recv.at[side, pair]).wait()

    def wait_sums(pair):
        with scope("w_sums"):
            each_side(lambda side: sums_wait(side, pair))

    def stack(start, stop):
        for a in range(start, stop):
            sums = sums_own[a] + sums_in[0, a].astype(f32) + sums_in[1, a].astype(f32)
            stacked[a, planes:] = sums.astype(bf16)

    def weigh_first():
        count_covers()
        for a in pairs[0]:
            weigh(a)

    def first_pair():
        wait_sums(0)
        load_gradient.start(priority=1)
        with scope("bwd"):
            stack(0, half)
            backward(0, half)

    def second_pair(angles_left):
        for a in angles_left:
            wait_tile(a)
        with scope("w_grad"):
            load_gradient.wait()
        wait_sums(1)
        with scope("bwd2"):
            gradient_sums[...] = fold_tile(gradient_vm[...] * gradient_vm[...])
            stack(half, angles)
            for a in angles_left:
                forward(a)
                weigh(a)
            backward(half, angles)
            image_total = image_sums[0]
            for a in range(1, angles):
                image_total = image_total + image_sums[a]
            parts = (gradient_sums[...], image_total, product_sums[0], product_sums[1], product_sums[2])
            stat_send[...] = jnp.concatenate([jnp.sum(x, axis=0, keepdims=True) for x in parts], axis=0)
        for d in range(1, count):
            pltpu.make_async_remote_copy(
                stat_send, stat_recv.at[d - 1], stat_sems.at[0], stat_sems.at[1],
                device_id={"slab": lax.rem(me + d, count)},
            ).start()

    @pl.when(late)
    def _():
        wait_tile(0)
        forward(0)
        take_covers()
        for a in range(1, half):
            forward_parts(a, (count_covers, functools.partial(weigh, 0)) if a == 1 else ())
            weigh(a)
        first_pair()
        second_pair(range(half, angles))

    @pl.when(jnp.logical_not(jnp.logical_or(early, late)))
    def _():
        for a in pairs[0]:
            forward_parts(a)
        take_covers()
        for a in range(half, last):
            forward_parts(a, (weigh_first,) if a == half else ())
            weigh(a)
        first_pair()
        second_pair(range(last, angles))

    @pl.when(early)
    def _():
        for a in pairs[0]:
            wait_tile(a)
            forward(a)
        take_covers()
        for a in range(half, angles):
            wait_tile(a)
            if a == half:
                weigh_first()
            forward(a)
            weigh(a)
        first_pair()
        second_pair(())

    with scope("w_halo"):
        each_side(lambda side: halo_copy(side).wait_send())
        each_side(lambda side: halo_copy(1 - side).wait_recv())

    with scope("fwdhalo"):
        for a in range(angles):
            image = jnp.dot(halo[...], tiles_vm[a], preferred_element_type=f32)
            for l in range(columns // LANES):
                cut = slice(l * LANES, (l + 1) * LANES)
                images[a, l, :planes] = image[:planes, cut]
                images[a, l, 2 * planes :] = image[planes:, cut]

    with scope("windows"):
        for j in range(per_angle):
            for a in range(angles):
                top = jnp.clip(offsets_sm[j * angles + a] + shift, 0, near - rows)
                for l in range(columns // LANES):
                    windows[j, a, :, l * LANES : (l + 1) * LANES] = images[a, l, pl.ds(top, rows), :]

    each_side(sums_sent)
    with scope("w_stat"):
        pltpu.make_async_copy(stat_recv, stat_recv, stat_sems.at[0]).wait()
        pltpu.make_async_copy(stat_recv, stat_recv, stat_sems.at[1]).wait()
    sums = stat_send[...]
    for d in range(1, count):
        sums = sums + stat_recv[d - 1]
    norms = jnp.sum(sums, axis=1, keepdims=True)
    grad_norm, image_norm = norms[0:1], norms[1:2]
    step_size = grad_norm / image_norm
    new_norm = norms[2:3] - 2.0 * step_size * norms[3:4] + step_size * step_size * norms[4:5]
    stats_out[...] = jnp.concatenate(
        [
            jnp.broadcast_to(step_size, (1, LANES)),
            jnp.broadcast_to(new_norm / grad_norm, (1, LANES)),
            jnp.zeros((6, LANES), f32),
        ],
        axis=0,
    )


def finish(
    stats, solution_ref, direction_ref, back_image, back_residual, windows, residual_ref,
    solution_out, residual_out, gradient_out, direction_out,
    volumes_vm, residual_vm, sems,
):
    per_angle, angles = residual_ref.shape[:2]
    step_size = stats[0:1, 0:1]
    scale = stats[1:2, 0:1]
    for j in range(per_angle):
        for a in range(angles):
            residual_vm[j, a] = residual_ref[j, a] - step_size * windows[j, a]
            pltpu.make_async_copy(residual_vm.at[j, a], residual_out.at[j, a], sems.at[0]).start()
    gradient = back_residual[...] - step_size * back_image[...]
    volumes_vm[0] = gradient
    pltpu.make_async_copy(volumes_vm.at[0], gradient_out, sems.at[1]).start()
    volumes_vm[1] = gradient + scale * direction_ref[...]
    pltpu.make_async_copy(volumes_vm.at[1], direction_out, sems.at[1]).start()
    volumes_vm[2] = solution_ref[...] + step_size * direction_ref[...]
    pltpu.make_async_copy(volumes_vm.at[2], solution_out, sems.at[1]).start()
    pltpu.make_async_copy(residual_vm, residual_out, sems.at[0]).wait()
    pltpu.make_async_copy(volumes_vm, volumes_vm, sems.at[1]).wait()


def local(count, solution, direction, gradient, residual, tiles, offsets):
    planes, cells = solution.shape
    views, rows, columns = residual.shape
    angles = tiles.shape[0]
    per_angle = views // angles
    near = 3 * planes
    half = angles // 2
    f32, bf16 = jnp.float32, jnp.bfloat16
    hbm = pl.BlockSpec(memory_space=pltpu.HBM)
    vmem = pl.BlockSpec(memory_space=pltpu.VMEM)
    dma = pltpu.SemaphoreType.DMA
    by_angle = residual.reshape(per_angle, angles, rows, columns)
    volume = jax.ShapeDtypeStruct((planes, cells), f32)
    detector = jax.ShapeDtypeStruct(by_angle.shape, f32)
    remote = [pltpu.with_memory_space_constraint(x, pltpu.HBM) for x in (offsets, direction, gradient, by_angle, tiles)]
    residual_in, windows, direction_in, back_image, back_residual, stats = pl.pallas_call(
        functools.partial(project, count),
        name="project",
        out_shape=(detector, detector, volume, volume, volume, jax.ShapeDtypeStruct((8, LANES), f32)),
        in_specs=[hbm] * 5,
        out_specs=(vmem,) * 6,
        scratch_shapes=[
            pltpu.SMEM((views,), jnp.int32),
            pltpu.VMEM((planes, cells), f32),
            pltpu.VMEM((angles, cells, columns), bf16),
            pltpu.VMEM((planes, cells), bf16),
            pltpu.VMEM((2 * planes, cells), bf16),
            pltpu.VMEM((angles, columns // LANES, near, LANES), f32),
            pltpu.VMEM((angles, near, per_angle * rows), bf16),
            pltpu.VMEM((near, LANES), bf16),
            pltpu.VMEM((2, planes, LANES), bf16),
            pltpu.VMEM((planes, angles * LANES), f32),
            pltpu.VMEM((angles, 8, LANES), f32),
            pltpu.VMEM((3, 8, LANES), f32),
            pltpu.VMEM((8, LANES), f32),
            pltpu.VMEM((angles, planes, columns), f32),
            pltpu.VMEM((2, angles, planes, columns), bf16),
            pltpu.VMEM((2, angles, planes, columns), bf16),
            pltpu.VMEM((angles, 2 * planes, columns), bf16),
            pltpu.VMEM((cells, 2 * planes), f32),
            pltpu.VMEM((STATS, LANES), f32),
            pltpu.VMEM((count - 1, STATS, LANES), f32),
            dma((2,)),
            dma((half + 1,)),
            dma((2 * angles - 3,)),
            dma((2,)),
            dma((2,)),
            dma((2,)),
            dma((2, 2)),
            dma((2,)),
            dma((2,)),
        ],
        compiler_params=pltpu.CompilerParams(
            collective_id=0,
            has_side_effects=True,
            vmem_limit_bytes=PROJECT_MIB * 1024 * 1024,
        ),
    )(*remote)
    results = pl.pallas_call(
        finish,
        name="finish",
        out_shape=(volume, detector, volume, volume),
        in_specs=[vmem] * 7,
        out_specs=(hbm,) * 4,
        scratch_shapes=[
            pltpu.VMEM((3, planes, cells), f32),
            pltpu.VMEM(by_angle.shape, f32),
            dma((2,)),
        ],
        compiler_params=pltpu.CompilerParams(vmem_limit_bytes=FINISH_MIB * 1024 * 1024),
    )(stats, solution, direction_in, back_image, back_residual, windows, residual_in)
    return results[0], results[1].reshape(residual.shape), results[2], results[3]


def solution(mesh):
    placed = (
        P(("scan", "slab"), None),
        P(("scan", "slab"), None),
        P(("scan", "slab"), None),
        P(("scan", "slab"), None, None),
        P(),
        P(("scan", "slab")),
    )
    return jax.shard_map(
        functools.partial(local, mesh.shape["slab"]),
        mesh=mesh,
        in_specs=placed,
        out_specs=(
            P(("scan", "slab"), None),
            P(("scan", "slab"), None, None),
            P(("scan", "slab"), None),
            P(("scan", "slab"), None),
        ),
        check_vma=False,
    )
```
